32 devices in a mesh: shot: 2 (over y), inline: 4 (over z), xline: 2 (over x), depth: 2 (over core).
Axes of the slice: x: 2, y: 2, z: 4, core: 2. Of those that a mesh axis runs over, the one named last changes fastest.
Arguments:
- forward_now: float32 [2, 32, 64, 256], P(None, ('shot', 'inline'), 'xline', 'depth'), parts along dimension 1, may hold values from -6 to 6
- forward_before: float32 [2, 32, 64, 256], P(None, ('shot', 'inline'), 'xline', 'depth'), parts along dimension 1, may hold values from -6 to 6
- adjoint_now: float32 [2, 32, 64, 256], P(None, ('shot', 'inline'), 'xline', 'depth'), parts along dimension 1, may hold values from -6 to 6
- adjoint_before: float32 [2, 32, 64, 256], P(None, ('shot', 'inline'), 'xline', 'depth'), parts along dimension 1, may hold values from -6 to 6
- courant: float32 [16, 64, 256], P('inline', 'xline', 'depth'), may hold values from 0.04 to 0.15
- thomsen_epsilon: float32 [16, 64, 256], P('inline', 'xline', 'depth'), may hold values from 0.2 to 0.4
- thomsen_delta: float32 [16, 64, 256], P('inline', 'xline', 'depth'), may hold values from 0 to 0.2
- tilt_class: int32 [16, 64, 256], P('inline', 'xline', 'depth'), may hold values from 0 to 15
- azimuth_class: int32 [16, 64, 256], P('inline', 'xline', 'depth'), may hold values from 0 to 31
- tilt_table: float32 [16], replicated, may hold values from -3.140625 to 3.140625
- azimuth_table: float32 [32], replicated, may hold values from -3.140625 to 3.140625
- source_cell: int32 [2], P('shot'), parts along dimension 0, may hold values from 0 to 262143
- wavelet: float32 [8], P('shot'), parts along dimension 0, may hold values from -6 to 6
- receiver_cells: int32 [4096], P('shot'), parts along dimension 0, may hold values from 0 to 262143
- receiver_data: float32 [4, 4096], P(None, 'shot'), parts along dimension 1, may hold values from -6 to 6
Outputs:
- forward_fields: float32 [2, 32, 64, 256], P(None, ('shot', 'inline'), 'xline', 'depth'), parts along dimension 1
- adjoint_fields: float32 [2, 32, 64, 256], P(None, ('shot', 'inline'), 'xline', 'depth'), parts along dimension 1
- migrated_image: float32 [32, 64, 256], P(('shot', 'inline'), 'xline', 'depth'), parts along dimension 0
- traces: float32 [4, 4096], P(None, 'shot'), parts along dimension 1
The draws below stay inside these ranges and needn't reach their ends.
There are 2 independent parts, one for each index of `shot`. The reference program is written for one: setup_inputs(seed, part) draws one part's arguments, and reference() takes and returns one part's arrays. A program takes and returns all parts, laid end to end along the dimension named above; an argument that names none is the same for every part. Nothing has to cross between parts.
All inputs are finite; a program needn't handle non-finite values.
Results may differ from the reference program's by a relative error of at most 0.00002.
Values sent between devices are 32-bit elements; how exact they have to be, the bound alone decides.
A program may use at most 128 MiB of HBM per device.

```python
import jax
import jax.numpy as jnp

CX = 4
CY = 32
CZ = 128
STEPS = 4
NREC = 2048
NTILT = 16
NAZ = 32
NX = 16
NY = 64
NZ = 256


def draw_forward_now(key, part):
    array_shape = (2, NX, NY, NZ)
    values = jnp.clip(jax.random.normal(key, array_shape, jnp.float32), -6.0, 6.0)
    return values


def draw_receiver_cells(key, part):
    inline_blocks = NX // CX
    xline_blocks = NY // CY
    depth_blocks = NZ // CZ
    block_count = inline_blocks * xline_blocks * depth_blocks
    spread_count = NREC // 2
    block_shift = jax.random.randint(jax.random.fold_in(key, 10), (), 0, block_count, jnp.int32)
    spread_block = (jnp.arange(spread_count, dtype=jnp.int32) + block_shift) % block_count
    inline_block = spread_block // (xline_blocks * depth_blocks)
    xline_block = spread_block // depth_blocks % xline_blocks
    depth_block = spread_block % depth_blocks
    inline_local = jax.random.randint(jax.random.fold_in(key, 11), (spread_count,), 0, CX, jnp.int32)
    xline_local = jax.random.randint(jax.random.fold_in(key, 12), (spread_count,), 0, CY, jnp.int32)
    depth_local = jax.random.randint(jax.random.fold_in(key, 13), (spread_count,), 0, CZ, jnp.int32)
    spread_cells = ((inline_block * CX + inline_local) * NY + xline_block * CY + xline_local) * NZ + depth_block * CZ + depth_local
    loose_count = NREC - spread_count
    loose_inline = jax.random.randint(jax.random.fold_in(key, 14), (loose_count,), 0, NX, jnp.int32)
    loose_xline = jax.random.randint(jax.random.fold_in(key, 15), (loose_count,), 0, NY, jnp.int32)
    loose_depth = jax.random.randint(jax.random.fold_in(key, 16), (loose_count,), 0, NZ, jnp.int32)
    loose_cells = (loose_inline * NY + loose_xline) * NZ + loose_depth
    every_cell = jnp.concatenate([spread_cells, loose_cells]).astype(jnp.int32)
    order = jax.random.permutation(jax.random.fold_in(key, 17), NREC)
    return every_cell[order].astype(jnp.int32)


def set_ends(array, own_key, smallest, largest):
    shape = array.shape
    index_at = [jax.random.randint(jax.random.fold_in(own_key, axis), (), 0, shape[axis]) for axis in range(len(shape))]
    array = array.at[tuple(index_at)].set(smallest)
    longest = shape.index(max(shape))
    index_at[longest] = (index_at[longest] + 1) % shape[longest]
    return array.at[tuple(index_at)].set(largest)


def level_of(rng, extent, shards, smallest, top_value):
    level, own = 1.0, jax.random.fold_in(rng, 6)
    for dim, parts in shards:
        heights = jnp.exp(jax.random.uniform(jax.random.fold_in(own, dim), (parts,), jnp.float32, smallest / len(shards), top_value / len(shards)))
        level = level * jnp.repeat(heights, extent[dim] // parts).reshape([-1 if axis == dim else 1 for axis in range(len(extent))])
    return level


def bell_draw(stream_key, shape, scale, limit, shards=(), kind=jnp.bfloat16):
    entries = jax.random.normal(stream_key, shape, jnp.float32) * scale
    if len(shards) > 0:
        entries = level_of(stream_key, shape, shards, -0.22, 0.18) * entries
    return jnp.clip(entries, min=-limit, max=limit).astype(kind)


def setup_inputs(seed: int = 0, part: int = 0) -> dict:
    streams_of = jax.random.split(jax.random.key(seed), 16)
    own_keys = jax.random.split(jax.random.fold_in(streams_of[15], part), 16)
    forward_now = draw_forward_now(jax.random.fold_in(jax.random.fold_in(streams_of[15], part), 71), part)
    forward_before = bell_draw(own_keys[1], (2, NX, NY, NZ), 1.0, 6.0, ((1, 4), (2, 2), (3, 2)), jnp.float32)
    adjoint_now = bell_draw(own_keys[2], (2, NX, NY, NZ), 1.0, 6.0, ((1, 4), (2, 2), (3, 2)), jnp.float32)
    adjoint_before = bell_draw(own_keys[3], (2, NX, NY, NZ), 1.0, 6.0, ((1, 4), (2, 2), (3, 2)), jnp.float32)
    courant = jnp.clip(0.04 + 0.11000001 * jax.random.uniform(streams_of[4], (NX, NY, NZ), jnp.float32) ** level_of(streams_of[4], (NX, NY, NZ), ((0, 4), (1, 2), (2, 2)), -0.2, 0.2), 0.04, 0.15)
    thomsen_epsilon = jnp.clip(0.2 + 0.2 * jax.random.uniform(streams_of[5], (NX, NY, NZ), jnp.float32) ** level_of(streams_of[5], (NX, NY, NZ), ((0, 4), (1, 2), (2, 2)), -0.2, 0.2), 0.2, 0.4)
    thomsen_delta = jnp.clip(0.2 * jax.random.uniform(streams_of[6], (NX, NY, NZ), jnp.float32) ** level_of(streams_of[6], (NX, NY, NZ), ((0, 4), (1, 2), (2, 2)), -0.2, 0.2), 0.0, 0.2)
    tilt_class = set_ends(jax.random.randint(streams_of[7], (NX, NY, NZ), 0, NTILT), jax.random.fold_in(streams_of[7], 1), 0, NTILT - 1).astype(jnp.int32)
    azimuth_class = set_ends(jax.random.randint(streams_of[8], (NX, NY, NZ), 0, NAZ), jax.random.fold_in(streams_of[8], 1), 0, NAZ - 1).astype(jnp.int32)
    tilt_table = jnp.clip(jax.random.uniform(streams_of[9], (NTILT,), jnp.float32, -3.140625, 3.140625), -3.140625, 3.140625)
    azimuth_table = jnp.clip(jax.random.uniform(streams_of[10], (NAZ,), jnp.float32, -3.140625, 3.140625), -3.140625, 3.140625)
    source_cell = jax.random.randint(own_keys[11], (1,), 0, NX * NY * NZ).astype(jnp.int32)
    wavelet = bell_draw(own_keys[12], (STEPS,), 1.0, 6.0, (), jnp.float32)
    receiver_cells = draw_receiver_cells(jax.random.fold_in(jax.random.fold_in(streams_of[15], part), 71), part)
    receiver_data = bell_draw(own_keys[14], (STEPS, NREC), 1.0, 6.0, (), jnp.float32)
    return dict(forward_now=forward_now, forward_before=forward_before, adjoint_now=adjoint_now, adjoint_before=adjoint_before, courant=courant, thomsen_epsilon=thomsen_epsilon, thomsen_delta=thomsen_delta, tilt_class=tilt_class, azimuth_class=azimuth_class, tilt_table=tilt_table, azimuth_table=azimuth_table, source_cell=source_cell, wavelet=wavelet, receiver_cells=receiver_cells, receiver_data=receiver_data)


def differences(padded):
    centre = padded[..., 1:-1, 1:-1, 1:-1]
    inline_inline = padded[..., 2:, 1:-1, 1:-1] + padded[..., :-2, 1:-1, 1:-1] - 2.0 * centre
    xline_xline = padded[..., 1:-1, 2:, 1:-1] + padded[..., 1:-1, :-2, 1:-1] - 2.0 * centre
    depth_depth = padded[..., 1:-1, 1:-1, 2:] + padded[..., 1:-1, 1:-1, :-2] - 2.0 * centre
    inline_xline = 0.25 * (padded[..., 2:, 2:, 1:-1] - padded[..., 2:, :-2, 1:-1] - padded[..., :-2, 2:, 1:-1] + padded[..., :-2, :-2, 1:-1])
    inline_depth = 0.25 * (padded[..., 2:, 1:-1, 2:] - padded[..., 2:, 1:-1, :-2] - padded[..., :-2, 1:-1, 2:] + padded[..., :-2, 1:-1, :-2])
    xline_depth = 0.25 * (padded[..., 1:-1, 2:, 2:] - padded[..., 1:-1, 2:, :-2] - padded[..., 1:-1, :-2, 2:] + padded[..., 1:-1, :-2, :-2])
    return centre, inline_inline, xline_xline, depth_depth, inline_xline, inline_depth, xline_depth


def advance_pair(padded, before, factors):
    centre, inline_inline, xline_xline, depth_depth, inline_xline, inline_depth, xline_depth = differences(padded)
    axial_part = (factors[3] * inline_inline + factors[4] * xline_xline + factors[5] * depth_depth
                  + factors[6] * inline_xline + factors[7] * inline_depth + factors[8] * xline_depth)
    plane_part = (inline_inline + xline_xline + depth_depth)[0] - axial_part[0]
    pressure = 2.0 * centre[0] - before[0] + factors[0] * plane_part + factors[2] * axial_part[1]
    auxiliary = 2.0 * centre[1] - before[1] + factors[1] * plane_part + factors[2] * axial_part[1]
    return jnp.stack([pressure, auxiliary])


def coefficients(courant, thomsen_epsilon, thomsen_delta, tilt_sine, tilt_cosine, azimuth_cosine, azimuth_sine):
    axis_first = tilt_sine * azimuth_cosine
    axis_second = tilt_sine * azimuth_sine
    axis_third = tilt_cosine
    return jnp.stack([courant * (1.0 + 2.0 * thomsen_epsilon), courant * (1.0 + 2.0 * thomsen_delta), courant,
                      axis_first * axis_first, axis_second * axis_second, axis_third * axis_third,
                      2.0 * axis_first * axis_second, 2.0 * axis_first * axis_third, 2.0 * axis_second * axis_third])


def reference(forward_now, forward_before, adjoint_now, adjoint_before, courant, thomsen_epsilon, thomsen_delta,
              tilt_class, azimuth_class, tilt_table, azimuth_table, source_cell, wavelet, receiver_cells, receiver_data):
    tilt_sine = jnp.sin(tilt_table)[tilt_class]
    tilt_cosine = jnp.cos(tilt_table)[tilt_class]
    azimuth_cosine = jnp.cos(azimuth_table)[azimuth_class]
    azimuth_sine = jnp.sin(azimuth_table)[azimuth_class]
    factors = coefficients(courant, thomsen_epsilon, thomsen_delta, tilt_sine, tilt_cosine, azimuth_cosine, azimuth_sine)
    forward_current, forward_previous = forward_now, forward_before
    adjoint_current, adjoint_previous = adjoint_now, adjoint_before
    volume = NX * NY * NZ
    padding = ((0, 0), (1, 1), (1, 1), (1, 1))
    image_sum = jnp.zeros((NX, NY, NZ), jnp.float32)
    records = []
    for moment in range(STEPS):
        forward_next = advance_pair(jnp.pad(forward_current, padding), forward_previous, factors)
        adjoint_next = advance_pair(jnp.pad(adjoint_current, padding), adjoint_previous, factors)
        source_term = jnp.zeros((volume,), jnp.float32).at[source_cell].add(
            jnp.broadcast_to(wavelet[moment], source_cell.shape)).reshape(NX, NY, NZ)
        receiver_term = jnp.zeros((volume,), jnp.float32).at[receiver_cells].add(
            receiver_data[moment]).reshape(NX, NY, NZ)
        forward_next = forward_next + source_term[None]
        adjoint_next = adjoint_next + receiver_term[None]
        records.append(forward_next[0].reshape(volume)[receiver_cells])
        image_sum = image_sum + forward_next[0] * adjoint_next[0] + forward_next[1] * adjoint_next[1]
        forward_previous, forward_current = forward_current, forward_next
        adjoint_previous, adjoint_current = adjoint_current, adjoint_next
    return forward_current, adjoint_current, image_sum, jnp.stack(records)
```

```python
import functools

import jax
import jax.numpy as jnp
from jax import lax
from jax.experimental import pallas as pl
from jax.experimental.pallas import tpu as pltpu
from jax.sharding import PartitionSpec as P

STEPS = 4
MESH = pl.DeviceIdType.MESH
AXES = ("inline", "xline", "depth")
LANES = 128
TOP = 8

DIRECTIONS = [
    (a, b, c)
    for a in (-1, 0, 1)
    for b in (-1, 0, 1)
    for c in (-1, 0, 1)
    if 1 <= abs(a) + abs(b) + abs(c) <= 2
]


def split_by(values, size):
    if size & (size - 1) == 0:
        return values >> (size.bit_length() - 1), values & (size - 1)
    quotient = lax.div(values, jnp.int32(size))
    return quotient, values - quotient * size


def three_parts(values):
    high = values.astype(jnp.bfloat16).astype(jnp.float32)
    rest = values - high
    middle = rest.astype(jnp.bfloat16).astype(jnp.float32)
    return high, middle, rest - middle


def kernel(
    sizes,
    forward_now,
    forward_before,
    adjoint_now,
    adjoint_before,
    courant,
    epsilon,
    delta,
    tilt_class,
    azimuth_class,
    tilt_table,
    azimuth_table,
    source_cell,
    wavelet,
    receiver_cells,
    receiver_data,
    forward_out,
    adjoint_out,
    image_out,
    traces_out,
    fields,
    model,
    classes,
    factors,
    zdiff,
    zsum,
    row_send,
    edge_send,
    row_got,
    depth_got,
    xy_got,
    xz_got,
    yz_got,
    hot_row,
    hot_lane,
    spread,
    terms,
    trace_own,
    trace_plane,
    trace_sum,
    trace_line,
    load_sem,
    halo_send,
    halo_recv,
    plane_send,
    plane_recv,
    line_send,
    line_recv,
):
    n_in, n_x, n_d = sizes
    _, cx, cy, cz = forward_now.shape
    nrec = receiver_cells.shape[1]
    groups = cy // 8
    here = tuple(lax.axis_index(axis) for axis in AXES)
    rows = slice(TOP, TOP + cy)

    def present(direction):
        ok = None
        for at, step, size in zip(here, direction, sizes):
            if step == 0:
                continue
            this = (at < size - 1) if step > 0 else (at > 0)
            ok = this if ok is None else jnp.logical_and(ok, this)
        return ok

    def target(direction):
        return {
            axis: at + step for axis, at, step in zip(AXES, here, direction) if step != 0
        }

    live = [d for d in DIRECTIONS if all(s == 0 or n > 1 for s, n in zip(d, sizes))]

    loads = []
    for number, (source, place) in enumerate(
        [
            (forward_now, fields.at[1, 0, :, pl.ds(1, cx), pl.ds(TOP, cy)]),
            (adjoint_now, fields.at[1, 1, :, pl.ds(1, cx), pl.ds(TOP, cy)]),
            (forward_before, fields.at[0, 0, :, pl.ds(1, cx), pl.ds(TOP, cy)]),
            (adjoint_before, fields.at[0, 1, :, pl.ds(1, cx), pl.ds(TOP, cy)]),
            (courant, model.at[0]),
            (epsilon, model.at[1]),
            (delta, model.at[2]),
            (tilt_class, classes.at[0]),
            (azimuth_class, classes.at[1]),
        ]
    ):
        load = pltpu.make_async_copy(source, place, load_sem.at[number])
        load.start()
        loads.append(load)

    barrier = pltpu.get_barrier_semaphore()

    def plane_peer(k):
        xline_at = lax.rem(here[1] + k // n_d, n_x)
        depth_at = lax.rem(here[2] + k % n_d, n_d)
        return {"xline": xline_at, "depth": depth_at}

    def line_peer(k):
        return {"inline": lax.rem(here[0] + k, n_in)}

    for k in range(1, n_x * n_d):
        pl.semaphore_signal(barrier, inc=1, device_id=plane_peer(k), device_id_type=MESH)
    for k in range(1, n_in):
        pl.semaphore_signal(barrier, inc=1, device_id=line_peer(k), device_id_type=MESH)
    crossing = [d for d in live if d[0] != 0 and (d[1] != 0 or d[2] != 0)]
    for d in crossing:

        @pl.when(present(d))
        def _(d=d):
            pl.semaphore_signal(barrier, inc=1, device_id=target(d), device_id_type=MESH)

    def got_ref(d, s, system):
        sides = [0 if step > 0 else 1 for step in d]
        if d[0] and not d[1] and not d[2]:
            plane = 0 if d[0] > 0 else cx + 1
            return fields.at[s + 1, system, :, plane, pl.ds(TOP, cy)]
        if d[1] and not d[0] and not d[2]:
            return row_got.at[s, system, sides[1]]
        if d[2] and not d[0] and not d[1]:
            return depth_got.at[s, system, sides[2]]
        if d[0] and d[1]:
            return xy_got.at[s, system, sides[0], sides[1]]
        if d[0] and d[2]:
            return xz_got.at[s, system, sides[0], sides[2]]
        return yz_got.at[s, system, sides[1], sides[2]]

    def clear(d):
        for s in range(STEPS):
            for system in range(2):
                place = got_ref(d, s, system)
                place[...] = jnp.zeros(place.shape, jnp.float32)

    for d in DIRECTIONS:
        if d not in live:
            clear(d)
        else:
            arrives = present(tuple(-step for step in d))

            @pl.when(jnp.logical_not(arrives))
            def _(d=d):
                clear(d)

    def sent_ref(d, s, system):
        if d[0] and not d[1] and not d[2]:
            plane = cx if d[0] > 0 else 1
            return fields.at[s + 1, system, :, plane, pl.ds(TOP, cy)]
        if d[2] and not d[0] and not d[1]:
            return fields.at[s + 1, system, :, pl.ds(1, cx), pl.ds(TOP, cy)]
        if d[1]:
            return row_send.at[s, system, 1 if d[1] > 0 else 0]
        return edge_send.at[s, system, 1 if d[0] > 0 else 0]

    def halo_copy(d, s, system):
        number = DIRECTIONS.index(d)
        return pltpu.make_async_remote_copy(
            src_ref=sent_ref(d, s, system),
            dst_ref=got_ref(d, s, system),
            send_sem=halo_send.at[s, system, number],
            recv_sem=halo_recv.at[s, system, number],
            device_id=target(d),
            device_id_type=MESH,
        )

    lane = lax.broadcasted_iota(jnp.int32, (8, LANES), 1)
    lane_plane = lax.broadcasted_iota(jnp.int32, (cy, LANES), 1)

    def stage(s, system):
        for side, plane in ((0, 1), (1, cx)):
            packed = jnp.zeros((8, LANES), jnp.float32)
            for f in range(2):
                for r in range(groups):
                    slot = f * groups + r
                    chunk = fields[s + 1, system, f, plane, TOP + 8 * r : TOP + 8 * r + 8, :]
                    packed = jnp.where(
                        lane == slot, pltpu.roll(chunk, (slot + 1) % LANES, 1), packed
                    )
                    other = 2 * groups + slot
                    packed = jnp.where(lane == other, pltpu.roll(chunk, other % LANES, 1), packed)
            edge_send[s, system, side] = packed
        for side, row in ((0, TOP), (1, TOP + cy - 1)):
            for f in range(2):
                for i in range(cx):
                    at = f * cx + i
                    row_send[s, system, side, at : at + 1, :] = fields[
                        s + 1, system, f, i + 1, row : row + 1, :
                    ]

    order = sorted(live, key=lambda d: (not (d[0] and not d[1] and not d[2]), d[0] == 0))

    def send(s, system):
        for d in order:

            @pl.when(present(d))
            def _(d=d):
                halo_copy(d, s, system).start()

    def receive(s, system):
        for d in order:

            @pl.when(present(tuple(-step for step in d)))
            def _(d=d):
                halo_copy(d, s, system).wait_recv()

    def drain(s, system):
        for d in order:

            @pl.when(present(d))
            def _(d=d):
                halo_copy(d, s, system).wait_send()

    def finish_halo(s, system):
        for side, row in ((0, TOP - 1), (1, TOP + cy)):
            tile = row_got[s, system, side]
            before = jnp.where(
                lax.broadcasted_iota(jnp.int32, tile.shape, 1) == LANES - 1,
                yz_got[s, system, side, 0],
                tile,
            )
            after = jnp.where(
                lax.broadcasted_iota(jnp.int32, tile.shape, 1) == 0,
                yz_got[s, system, side, 1],
                tile,
            )
            change = pltpu.roll(after, LANES - 1, 1) - pltpu.roll(before, 1, 1)
            for f in range(2):
                for i in range(cx):
                    at = f * cx + i
                    fields[s + 1, system, f, i + 1, row : row + 1, :] = tile[at : at + 1, :]
                    zdiff[f, i + 1, row : row + 1, :] = change[at : at + 1, :]
                for xside, plane, from_plane in ((0, 0, cx - 1), (1, cx + 1, 0)):
                    at = f * cx + from_plane
                    fields[s + 1, system, f, plane, row : row + 1, :] = xy_got[
                        s, system, xside, side, at : at + 1, :
                    ]
        for f in range(2):
            for i in range(cx):
                centre = fields[s + 1, system, f, i + 1, rows, :]
                before = jnp.where(
                    lane_plane == LANES - 1, depth_got[s, system, 0, f, i], centre
                )
                after = jnp.where(lane_plane == 0, depth_got[s, system, 1, f, i], centre)
                before = pltpu.roll(before, 1, 1)
                after = pltpu.roll(after, LANES - 1, 1)
                zdiff[f, i + 1, rows, :] = after - before
                zsum[f, i] = after + before
            for xside, plane in ((0, 0), (1, cx + 1)):
                low = xz_got[s, system, xside, 0]
                high = xz_got[s, system, xside, 1]
                for r in range(groups):
                    slot = f * groups + r
                    at = slice(TOP + 8 * r, TOP + 8 * r + 8)
                    chunk = fields[s + 1, system, f, plane, at, :]
                    before = jnp.where(
                        lane == 0,
                        pltpu.roll(low, (-slot) % LANES, 1),
                        pltpu.roll(chunk, 1, 1),
                    )
                    after = jnp.where(
                        lane == LANES - 1,
                        pltpu.roll(high, (LANES - 1 - 2 * groups - slot) % LANES, 1),
                        pltpu.roll(chunk, LANES - 1, 1),
                    )
                    zdiff[f, plane, at, :] = after - before

    up = slice(TOP - 1, TOP + cy - 1)
    down = slice(TOP + 1, TOP + cy + 1)

    def advance(s, system):
        for i in range(cx):
            axial = []
            lap = None
            for f in range(2):
                now = fields.at[s + 1, system, f]
                centre = now[i + 1, rows, :]
                twice = 2.0 * centre
                dxx = now[i + 2, rows, :] + now[i, rows, :] - twice
                dyy = now[i + 1, down, :] + now[i + 1, up, :] - twice
                dzz = zsum[f, i] - twice
                dxy = (
                    now[i + 2, down, :]
                    - now[i + 2, up, :]
                    - now[i, down, :]
                    + now[i, up, :]
                )
                dxz = zdiff[f, i + 2, rows, :] - zdiff[f, i, rows, :]
                dyz = zdiff[f, i + 1, down, :] - zdiff[f, i + 1, up, :]
                axial.append(
                    factors[3, i] * dxx
                    + factors[4, i] * dyy
                    + factors[5, i] * dzz
                    + factors[6, i] * dxy
                    + factors[7, i] * dxz
                    + factors[8, i] * dyz
                )
                if f == 0:
                    lap = dxx + dyy + dzz
            plane_part = lap - axial[0]
            along = factors[2, i] * axial[1]
            if system == 0:
                row_at = lax.broadcasted_iota(jnp.int32, (cy, LANES), 0)
                cell = (
                    (here[0] * cx + i) * (n_x * cy) + here[1] * cy + row_at
                ) * (n_d * cz) + here[2] * cz + lane_plane
                added = jnp.where(cell == source_cell[0], wavelet[s], 0.0)
            else:
                added = terms[s, i]
            new = []
            for f in range(2):
                value = (
                    2.0 * fields[s + 1, system, f, i + 1, rows, :]
                    - fields[s, system, f, i + 1, rows, :]
                    + factors[f, i] * plane_part
                    + along
                    + added
                )
                fields[s + 2, system, f, i + 1, rows, :] = value
                new.append(value)
            if system == 1:
                product = (
                    fields[s + 2, 0, 0, i + 1, rows, :] * new[0]
                    + fields[s + 2, 0, 1, i + 1, rows, :] * new[1]
                )
                if s == 0:
                    image_out[i] = product
                else:
                    image_out[i] = image_out[i] + product
            if s == STEPS - 1:
                out = forward_out if system == 0 else adjoint_out
                out[0, i] = new[0]
                out[1, i] = new[1]

    def coefficients():
        tilt_sine, tilt_cosine = jnp.sin(tilt_table[...]), jnp.cos(tilt_table[...])
        turn_sine, turn_cosine = jnp.sin(azimuth_table[...]), jnp.cos(azimuth_table[...])

        def look(which, i, tables):
            chosen = classes[which, i]
            found = [jnp.zeros((cy, LANES), jnp.float32) for _ in tables]
            for k in range(tables[0].shape[1]):
                match = chosen == k
                found = [
                    jnp.where(match, jnp.broadcast_to(t[:, k : k + 1], (cy, LANES)), v)
                    for t, v in zip(tables, found)
                ]
            return found

        for i in range(cx):
            sine, third = look(0, i, (tilt_sine, tilt_cosine))
            turned, across = look(1, i, (turn_cosine, turn_sine))
            first, second = sine * turned, sine * across
            base = model[0, i]
            factors[0, i] = base * (1.0 + 2.0 * model[1, i])
            factors[1, i] = base * (1.0 + 2.0 * model[2, i])
            factors[2, i] = base
            factors[3, i] = first * first
            factors[4, i] = second * second
            factors[5, i] = third * third
            factors[6, i] = 0.5 * first * second
            factors[7, i] = 0.5 * first * third
            factors[8, i] = 0.5 * second * third

    def receivers():
        cells = receiver_cells[...]
        upper, depth_at = split_by(cells, n_d * cz)
        inline_at, xline_at = split_by(upper, n_x * cy)
        inline_at = inline_at - here[0] * cx
        xline_at = xline_at - here[1] * cy
        depth_at = depth_at - here[2] * cz
        inside = (
            (inline_at >= 0)
            & (inline_at < cx)
            & (xline_at >= 0)
            & (xline_at < cy)
            & (depth_at >= 0)
            & (depth_at < cz)
        )
        row_of = jnp.where(inside, inline_at * cy + xline_at, -1)
        lane_of = jnp.where(inside, depth_at, -1)
        row_match = (
            lax.broadcasted_iota(jnp.int32, (cx * cy, nrec), 0)
            == jnp.broadcast_to(row_of, (cx * cy, nrec))
        )
        lane_match = (
            lax.broadcasted_iota(jnp.int32, (cz, nrec), 0)
            == jnp.broadcast_to(lane_of, (cz, nrec))
        )
        hot_row[...] = jnp.where(row_match, 1.0, 0.0)
        lanes_hot = jnp.where(lane_match, 1.0, 0.0).astype(jnp.bfloat16)
        for part in range(3):
            hot_lane[part * cz : (part + 1) * cz, :] = lanes_hot
        parts = three_parts(receiver_data[...])
        volume = cx * cy
        for s in range(STEPS):
            for number, part in enumerate(parts):
                start = (s * 3 + number) * volume
                spread[start : start + volume, :] = (
                    hot_row[...] * jnp.broadcast_to(part[s : s + 1, :], (volume, nrec))
                ).astype(jnp.bfloat16)
            got = lax.dot_general(
                spread[s * 3 * volume : (s + 1) * 3 * volume, :],
                hot_lane[0:cz, :],
                (((1,), (1,)), ((), ())),
                preferred_element_type=jnp.float32,
            )
            total = got[:volume] + got[volume : 2 * volume] + got[2 * volume :]
            for i in range(cx):
                terms[s, i] = total[i * cy : (i + 1) * cy, :]

    def sample(s):
        planes = [fields[s + 2, 0, 0, i + 1, rows, :] for i in range(cx)]
        field = jnp.concatenate(planes, axis=0)
        parts = jnp.concatenate([p.astype(jnp.bfloat16) for p in three_parts(field)], axis=1)
        picked = jnp.dot(parts, hot_lane[...], preferred_element_type=jnp.float32)
        trace_own[s] = jnp.sum(picked * hot_row[...], axis=0, keepdims=True)

    def plane_copy(s, k):
        return pltpu.make_async_remote_copy(
            src_ref=trace_own.at[s],
            dst_ref=trace_plane.at[s, k],
            send_sem=plane_send.at[s, k],
            recv_sem=plane_recv.at[s, k],
            device_id=plane_peer(k),
            device_id_type=MESH,
        )

    def line_copy(s, k):
        return pltpu.make_async_remote_copy(
            src_ref=trace_sum.at[s],
            dst_ref=trace_line.at[s, k],
            send_sem=line_send.at[s, k],
            recv_sem=line_recv.at[s, k],
            device_id=line_peer(k),
            device_id_type=MESH,
        )

    def share_plane(s):
        for k in range(1, n_x * n_d):
            plane_copy(s, k).start()

    def share_line(s):
        total = trace_own[s]
        for k in range(1, n_x * n_d):
            plane_copy(s, k).wait_recv()
            total = total + trace_plane[s, k]
        trace_sum[s] = total
        for k in range(1, n_in):
            line_copy(s, k).start()

    def finish_trace(s):
        total = trace_sum[s]
        for k in range(1, n_in):
            line_copy(s, k).wait_recv()
            total = total + trace_line[s, k]
        traces_out[s : s + 1, :] = total

    expected = jnp.int32(n_x * n_d - 1 + n_in - 1)
    for d in crossing:
        expected = expected + jnp.where(present(d), 1, 0)
    loads[0].wait()
    stage(0, 0)
    loads[1].wait()
    stage(0, 1)
    pl.semaphore_wait(barrier, expected)
    send(0, 0)
    send(0, 1)
    for load in loads[2:]:
        load.wait()
    coefficients()
    receivers()
    for s in range(STEPS):
        for system in range(2):
            receive(s, system)
            finish_halo(s, system)
            advance(s, system)
            if s < STEPS - 1:
                stage(s + 1, system)
                send(s + 1, system)
        sample(s)
        share_plane(s)
        if s > 0:
            share_line(s - 1)
    share_line(STEPS - 1)
    for s in range(STEPS):
        finish_trace(s)
    for s in range(STEPS):
        for system in range(2):
            drain(s, system)
        for k in range(1, n_x * n_d):
            plane_copy(s, k).wait_send()
        for k in range(1, n_in):
            line_copy(s, k).wait_send()


def per_device(sizes, *operands):
    shapes = [operand.shape for operand in operands]
    _, cx, cy, cz = shapes[0]
    nrec = shapes[13][0]
    n_in, n_x, n_d = sizes
    operands = list(operands)
    for which in (9, 10, 13):
        operands[which] = operands[which].reshape(1, -1)
    f32, bf16 = jnp.float32, jnp.bfloat16
    padded = cy + 2 * TOP
    combos = 2 * cx
    scratch = [
        pltpu.VMEM((STEPS + 2, 2, 2, cx + 2, padded, cz), f32),
        pltpu.VMEM((3, cx, cy, cz), f32),
        pltpu.VMEM((2, cx, cy, cz), jnp.int32),
        pltpu.VMEM((9, cx, cy, cz), f32),
        pltpu.VMEM((2, cx + 2, padded, cz), f32),
        pltpu.VMEM((2, cx, cy, cz), f32),
        pltpu.VMEM((STEPS, 2, 2, combos, cz), f32),
        pltpu.VMEM((STEPS, 2, 2, 8, cz), f32),
        pltpu.VMEM((STEPS, 2, 2, combos, cz), f32),
        pltpu.VMEM((STEPS, 2, 2, 2, cx, cy, cz), f32),
        pltpu.VMEM((STEPS, 2, 2, 2, combos, cz), f32),
        pltpu.VMEM((STEPS, 2, 2, 2, 8, cz), f32),
        pltpu.VMEM((STEPS, 2, 2, 2, combos, cz), f32),
        pltpu.VMEM((cx * cy, nrec), f32),
        pltpu.VMEM((3 * cz, nrec), bf16),
        pltpu.VMEM((3 * STEPS * cx * cy, nrec), bf16),
        pltpu.VMEM((STEPS, cx, cy, cz), f32),
        pltpu.VMEM((STEPS, 1, nrec), f32),
        pltpu.VMEM((STEPS, n_x * n_d, 1, nrec), f32),
        pltpu.VMEM((STEPS, 1, nrec), f32),
        pltpu.VMEM((STEPS, n_in, 1, nrec), f32),
        pltpu.SemaphoreType.DMA((9,)),
        pltpu.SemaphoreType.DMA((STEPS, 2, len(DIRECTIONS))),
        pltpu.SemaphoreType.DMA((STEPS, 2, len(DIRECTIONS))),
        pltpu.SemaphoreType.DMA((STEPS, n_x * n_d)),
        pltpu.SemaphoreType.DMA((STEPS, n_x * n_d)),
        pltpu.SemaphoreType.DMA((STEPS, n_in)),
        pltpu.SemaphoreType.DMA((STEPS, n_in)),
    ]
    vmem = pl.BlockSpec(memory_space=pltpu.VMEM)
    smem = pl.BlockSpec(memory_space=pltpu.SMEM)
    anywhere = pl.BlockSpec(memory_space=pl.ANY)
    return pl.pallas_call(
        functools.partial(kernel, sizes),
        out_shape=(
            jax.ShapeDtypeStruct((2, cx, cy, cz), f32),
            jax.ShapeDtypeStruct((2, cx, cy, cz), f32),
            jax.ShapeDtypeStruct((cx, cy, cz), f32),
            jax.ShapeDtypeStruct((STEPS, nrec), f32),
        ),
        in_specs=[anywhere] * 9 + [vmem, vmem, smem, smem, vmem, vmem],
        out_specs=(vmem, vmem, vmem, vmem),
        scratch_shapes=scratch,
        compiler_params=pltpu.CompilerParams(
            collective_id=0, has_side_effects=True, vmem_limit_bytes=56 * 2**20
        ),
        name="wavefields",
    )(*operands)


def solution(mesh):
    sizes = tuple(mesh.shape[axis] for axis in AXES)
    field = P(None, ("shot", "inline"), "xline", "depth")
    cell = P("inline", "xline", "depth")
    return jax.shard_map(
        functools.partial(per_device, sizes),
        mesh=mesh,
        in_specs=(
            field, field, field, field,
            cell, cell, cell, cell, cell,
            P(), P(), P("shot"), P("shot"), P("shot"), P(None, "shot"),
        ),
        out_specs=(field, field, P(("shot", "inline"), "xline", "depth"), P(None, "shot")),
        check_vma=False,
    )
```

```python
import functools

import jax
import jax.numpy as jnp
from jax import lax
from jax.experimental import pallas as pl
from jax.experimental.pallas import tpu as pltpu
from jax.sharding import PartitionSpec as P

STEPS = 4
MESH = pl.DeviceIdType.MESH
AXES = ("inline", "xline", "depth")
LANES = 128
TOP = 8

DIRECTIONS = [
    (a, b, c)
    for a in (-1, 0, 1)
    for b in (-1, 0, 1)
    for c in (-1, 0, 1)
    if 1 <= abs(a) + abs(b) + abs(c) <= 2
]


def split_by(values, size):
    if size & (size - 1) == 0:
        return values >> (size.bit_length() - 1), values & (size - 1)
    quotient = lax.div(values, jnp.int32(size))
    return quotient, values - quotient * size


def three_parts(values):
    high = values.astype(jnp.bfloat16).astype(jnp.float32)
    rest = values - high
    middle = rest.astype(jnp.bfloat16).astype(jnp.float32)
    return high, middle, rest - middle


def kernel(
    sizes,
    forward_now,
    forward_before,
    adjoint_now,
    adjoint_before,
    courant,
    epsilon,
    delta,
    tilt_class,
    azimuth_class,
    tilt_table,
    azimuth_table,
    source_cell,
    wavelet,
    receiver_cells,
    receiver_data,
    forward_out,
    adjoint_out,
    image_out,
    traces_out,
    fields,
    model,
    classes,
    factors,
    zdiff,
    zsum,
    row_send,
    row_edge,
    edge_send,
    row_got,
    depth_got,
    xy_got,
    xz_got,
    yz_got,
    hot_row,
    hot_lane,
    spread,
    terms,
    trace_own,
    trace_plane,
    trace_sum,
    trace_line,
    load_sem,
    halo_send,
    halo_recv,
    plane_send,
    plane_recv,
    line_send,
    line_recv,
):
    n_in, n_x, n_d = sizes
    _, cx, cy, cz = forward_now.shape
    nrec = receiver_cells.shape[1]
    groups = cy // 8
    here = tuple(lax.axis_index(axis) for axis in AXES)
    rows = slice(TOP, TOP + cy)

    def present(direction):
        ok = None
        for at, step, size in zip(here, direction, sizes):
            if step == 0:
                continue
            this = (at < size - 1) if step > 0 else (at > 0)
            ok = this if ok is None else jnp.logical_and(ok, this)
        return ok

    def target(direction):
        return {
            axis: at + step for axis, at, step in zip(AXES, here, direction) if step != 0
        }

    live = [d for d in DIRECTIONS if all(s == 0 or n > 1 for s, n in zip(d, sizes))]

    loads = []
    for number, (source, place) in enumerate(
        [
            (forward_now, fields.at[1, 0, :, pl.ds(1, cx), pl.ds(TOP, cy)]),
            (adjoint_now, fields.at[1, 1, :, pl.ds(1, cx), pl.ds(TOP, cy)]),
            (forward_before, fields.at[0, 0, :, pl.ds(1, cx), pl.ds(TOP, cy)]),
            (adjoint_before, fields.at[0, 1, :, pl.ds(1, cx), pl.ds(TOP, cy)]),
            (courant, model.at[0]),
            (epsilon, model.at[1]),
            (delta, model.at[2]),
            (tilt_class, classes.at[0]),
            (azimuth_class, classes.at[1]),
        ]
    ):
        load = pltpu.make_async_copy(source, place, load_sem.at[number])
        load.start()
        loads.append(load)

    barrier = pltpu.get_barrier_semaphore()

    def plane_peer(k):
        xline_at = lax.rem(here[1] + k // n_d, n_x)
        depth_at = lax.rem(here[2] + k % n_d, n_d)
        return {"xline": xline_at, "depth": depth_at}

    def line_peer(k):
        return {"inline": lax.rem(here[0] + k, n_in)}

    for k in range(1, n_x * n_d):
        pl.semaphore_signal(barrier, inc=1, device_id=plane_peer(k), device_id_type=MESH)
    for k in range(1, n_in):
        pl.semaphore_signal(barrier, inc=1, device_id=line_peer(k), device_id_type=MESH)
    crossing = [d for d in live if d[0] != 0 and (d[1] != 0 or d[2] != 0)]
    for d in crossing:

        @pl.when(present(d))
        def _(d=d):
            pl.semaphore_signal(barrier, inc=1, device_id=target(d), device_id_type=MESH)

    def got_ref(d, s, system):
        sides = [0 if step > 0 else 1 for step in d]
        if d[0] and not d[1] and not d[2]:
            plane = 0 if d[0] > 0 else cx + 1
            return fields.at[s + 1, system, :, plane, pl.ds(TOP, cy)]
        if d[1] and not d[0] and not d[2]:
            return row_got.at[s, system, sides[1]]
        if d[2] and not d[0] and not d[1]:
            return depth_got.at[s, system, sides[2]]
        if d[0] and d[1]:
            return xy_got.at[s, system, sides[0], sides[1]]
        if d[0] and d[2]:
            return xz_got.at[s, system, sides[0], sides[2]]
        return yz_got.at[s, system, sides[1], sides[2]]

    def clear(d):
        for s in range(STEPS):
            for system in range(2):
                place = got_ref(d, s, system)
                place[...] = jnp.zeros(place.shape, jnp.float32)

    for d in DIRECTIONS:
        if d not in live:
            clear(d)
        else:
            arrives = present(tuple(-step for step in d))

            @pl.when(jnp.logical_not(arrives))
            def _(d=d):
                clear(d)

    def sent_ref(d, s, system):
        if d[0] and not d[1] and not d[2]:
            plane = cx if d[0] > 0 else 1
            return fields.at[s + 1, system, :, plane, pl.ds(TOP, cy)]
        if d[2] and not d[0] and not d[1]:
            return fields.at[s + 1, system, :, pl.ds(1, cx), pl.ds(TOP, cy)]
        if d[0] and d[1]:
            return row_edge.at[s, system, 1 if d[1] > 0 else 0]
        if d[1]:
            return row_send.at[s, system, 1 if d[1] > 0 else 0]
        return edge_send.at[s, system, 1 if d[0] > 0 else 0]

    def halo_copy(d, s, system):
        number = DIRECTIONS.index(d)
        return pltpu.make_async_remote_copy(
            src_ref=sent_ref(d, s, system),
            dst_ref=got_ref(d, s, system),
            send_sem=halo_send.at[s, system, number],
            recv_sem=halo_recv.at[s, system, number],
            device_id=target(d),
            device_id_type=MESH,
        )

    lane = lax.broadcasted_iota(jnp.int32, (8, LANES), 1)
    lane_plane = lax.broadcasted_iota(jnp.int32, (cy, LANES), 1)

    def stage_edges(s, system):
        for side, plane in ((0, 1), (1, cx)):
            packed = jnp.zeros((8, LANES), jnp.float32)
            for f in range(2):
                for r in range(groups):
                    slot = f * groups + r
                    chunk = fields[s + 1, system, f, plane, TOP + 8 * r : TOP + 8 * r + 8, :]
                    packed = jnp.where(
                        lane == slot, pltpu.roll(chunk, (slot + 1) % LANES, 1), packed
                    )
                    other = 2 * groups + slot
                    packed = jnp.where(lane == other, pltpu.roll(chunk, other % LANES, 1), packed)
            edge_send[s, system, side] = packed
        for side, row in ((0, TOP), (1, TOP + cy - 1)):
            row_edge[s, system, side] = jnp.zeros(row_edge.shape[3:], jnp.float32)
            for f in range(2):
                for i in sorted({0, cx - 1}):
                    at = f * cx + i
                    row_edge[s, system, side, at : at + 1, :] = fields[
                        s + 1, system, f, i + 1, row : row + 1, :
                    ]

    def stage_rows(s, system):
        for side, row in ((0, TOP), (1, TOP + cy - 1)):
            for f in range(2):
                for i in range(cx):
                    at = f * cx + i
                    row_send[s, system, side, at : at + 1, :] = fields[
                        s + 1, system, f, i + 1, row : row + 1, :
                    ]

    order = sorted(live, key=lambda d: (not (d[0] and not d[1] and not d[2]), d[0] == 0))
    early = [d for d in order if d[0] != 0]
    late = [d for d in order if d[0] == 0]

    def send(s, system, which):
        for d in which:

            @pl.when(present(d))
            def _(d=d):
                halo_copy(d, s, system).start()

    def receive(s, system):
        for d in order:

            @pl.when(present(tuple(-step for step in d)))
            def _(d=d):
                halo_copy(d, s, system).wait_recv()

    def drain(s, system):
        for d in order:

            @pl.when(present(d))
            def _(d=d):
                halo_copy(d, s, system).wait_send()

    def finish_halo(s, system):
        for side, row in ((0, TOP - 1), (1, TOP + cy)):
            tile = row_got[s, system, side]
            before = jnp.where(
                lax.broadcasted_iota(jnp.int32, tile.shape, 1) == LANES - 1,
                yz_got[s, system, side, 0],
                tile,
            )
            after = jnp.where(
                lax.broadcasted_iota(jnp.int32, tile.shape, 1) == 0,
                yz_got[s, system, side, 1],
                tile,
            )
            change = pltpu.roll(after, LANES - 1, 1) - pltpu.roll(before, 1, 1)
            for f in range(2):
                for i in range(cx):
                    at = f * cx + i
                    fields[s + 1, system, f, i + 1, row : row + 1, :] = tile[at : at + 1, :]
                    zdiff[f, i + 1, row : row + 1, :] = change[at : at + 1, :]
                for xside, plane, from_plane in ((0, 0, cx - 1), (1, cx + 1, 0)):
                    at = f * cx + from_plane
                    fields[s + 1, system, f, plane, row : row + 1, :] = xy_got[
                        s, system, xside, side, at : at + 1, :
                    ]
        for f in range(2):
            for i in range(cx):
                centre = fields[s + 1, system, f, i + 1, rows, :]
                before = jnp.where(
                    lane_plane == LANES - 1, depth_got[s, system, 0, f, i], centre
                )
                after = jnp.where(lane_plane == 0, depth_got[s, system, 1, f, i], centre)
                before = pltpu.roll(before, 1, 1)
                after = pltpu.roll(after, LANES - 1, 1)
                zdiff[f, i + 1, rows, :] = after - before
                zsum[f, i] = after + before
            for xside, plane in ((0, 0), (1, cx + 1)):
                low = xz_got[s, system, xside, 0]
                high = xz_got[s, system, xside, 1]
                for r in range(groups):
                    slot = f * groups + r
                    at = slice(TOP + 8 * r, TOP + 8 * r + 8)
                    chunk = fields[s + 1, system, f, plane, at, :]
                    before = jnp.where(
                        lane == 0,
                        pltpu.roll(low, (-slot) % LANES, 1),
                        pltpu.roll(chunk, 1, 1),
                    )
                    after = jnp.where(
                        lane == LANES - 1,
                        pltpu.roll(high, (LANES - 1 - 2 * groups - slot) % LANES, 1),
                        pltpu.roll(chunk, LANES - 1, 1),
                    )
                    zdiff[f, plane, at, :] = after - before

    up = slice(TOP - 1, TOP + cy - 1)
    down = slice(TOP + 1, TOP + cy + 1)

    outer = sorted({0, cx - 1})
    inner = [i for i in range(cx) if i not in outer]

    def advance(s, system, planes):
        for i in planes:
            axial = []
            lap = None
            for f in range(2):
                now = fields.at[s + 1, system, f]
                centre = now[i + 1, rows, :]
                twice = 2.0 * centre
                dxx = now[i + 2, rows, :] + now[i, rows, :] - twice
                dyy = now[i + 1, down, :] + now[i + 1, up, :] - twice
                dzz = zsum[f, i] - twice
                dxy = (
                    now[i + 2, down, :]
                    - now[i + 2, up, :]
                    - now[i, down, :]
                    + now[i, up, :]
                )
                dxz = zdiff[f, i + 2, rows, :] - zdiff[f, i, rows, :]
                dyz = zdiff[f, i + 1, down, :] - zdiff[f, i + 1, up, :]
                axial.append(
                    factors[3, i] * dxx
                    + factors[4, i] * dyy
                    + factors[5, i] * dzz
                    + factors[6, i] * dxy
                    + factors[7, i] * dxz
                    + factors[8, i] * dyz
                )
                if f == 0:
                    lap = dxx + dyy + dzz
            plane_part = lap - axial[0]
            along = factors[2, i] * axial[1]
            if system == 0:
                row_at = lax.broadcasted_iota(jnp.int32, (cy, LANES), 0)
                cell = (
                    (here[0] * cx + i) * (n_x * cy) + here[1] * cy + row_at
                ) * (n_d * cz) + here[2] * cz + lane_plane
                added = jnp.where(cell == source_cell[0], wavelet[s], 0.0)
            else:
                added = terms[s, i]
            new = []
            for f in range(2):
                value = (
                    2.0 * fields[s + 1, system, f, i + 1, rows, :]
                    - fields[s, system, f, i + 1, rows, :]
                    + factors[f, i] * plane_part
                    + along
                    + added
                )
                fields[s + 2, system, f, i + 1, rows, :] = value
                new.append(value)
            if system == 1:
                product = (
                    fields[s + 2, 0, 0, i + 1, rows, :] * new[0]
                    + fields[s + 2, 0, 1, i + 1, rows, :] * new[1]
                )
                if s == 0:
                    image_out[i] = product
                else:
                    image_out[i] = image_out[i] + product
            if s == STEPS - 1:
                out = forward_out if system == 0 else adjoint_out
                out[0, i] = new[0]
                out[1, i] = new[1]

    def coefficients():
        tilt_sine, tilt_cosine = jnp.sin(tilt_table[...]), jnp.cos(tilt_table[...])
        turn_sine, turn_cosine = jnp.sin(azimuth_table[...]), jnp.cos(azimuth_table[...])

        def look(which, i, tables):
            chosen = classes[which, i]
            found = [jnp.zeros((cy, LANES), jnp.float32) for _ in tables]
            for k in range(tables[0].shape[1]):
                match = chosen == k
                found = [
                    jnp.where(match, jnp.broadcast_to(t[:, k : k + 1], (cy, LANES)), v)
                    for t, v in zip(tables, found)
                ]
            return found

        for i in range(cx):
            sine, third = look(0, i, (tilt_sine, tilt_cosine))
            turned, across = look(1, i, (turn_cosine, turn_sine))
            first, second = sine * turned, sine * across
            base = model[0, i]
            factors[0, i] = base * (1.0 + 2.0 * model[1, i])
            factors[1, i] = base * (1.0 + 2.0 * model[2, i])
            factors[2, i] = base
            factors[3, i] = first * first
            factors[4, i] = second * second
            factors[5, i] = third * third
            factors[6, i] = 0.5 * first * second
            factors[7, i] = 0.5 * first * third
            factors[8, i] = 0.5 * second * third

    def receivers():
        cells = receiver_cells[...]
        upper, depth_at = split_by(cells, n_d * cz)
        inline_at, xline_at = split_by(upper, n_x * cy)
        inline_at = inline_at - here[0] * cx
        xline_at = xline_at - here[1] * cy
        depth_at = depth_at - here[2] * cz
        inside = (
            (inline_at >= 0)
            & (inline_at < cx)
            & (xline_at >= 0)
            & (xline_at < cy)
            & (depth_at >= 0)
            & (depth_at < cz)
        )
        row_of = jnp.where(inside, inline_at * cy + xline_at, -1)
        lane_of = jnp.where(inside, depth_at, -1)
        row_match = (
            lax.broadcasted_iota(jnp.int32, (cx * cy, nrec), 0)
            == jnp.broadcast_to(row_of, (cx * cy, nrec))
        )
        lane_match = (
            lax.broadcasted_iota(jnp.int32, (cz, nrec), 0)
            == jnp.broadcast_to(lane_of, (cz, nrec))
        )
        hot_row[...] = jnp.where(row_match, 1.0, 0.0)
        lanes_hot = jnp.where(lane_match, 1.0, 0.0).astype(jnp.bfloat16)
        for part in range(3):
            hot_lane[part * cz : (part + 1) * cz, :] = lanes_hot
        parts = three_parts(receiver_data[...])
        volume = cx * cy
        for s in range(STEPS):
            for number, part in enumerate(parts):
                start = (s * 3 + number) * volume
                spread[start : start + volume, :] = (
                    hot_row[...] * jnp.broadcast_to(part[s : s + 1, :], (volume, nrec))
                ).astype(jnp.bfloat16)
            got = lax.dot_general(
                spread[s * 3 * volume : (s + 1) * 3 * volume, :],
                hot_lane[0:cz, :],
                (((1,), (1,)), ((), ())),
                preferred_element_type=jnp.float32,
            )
            total = got[:volume] + got[volume : 2 * volume] + got[2 * volume :]
            for i in range(cx):
                terms[s, i] = total[i * cy : (i + 1) * cy, :]

    def sample(s):
        planes = [fields[s + 2, 0, 0, i + 1, rows, :] for i in range(cx)]
        field = jnp.concatenate(planes, axis=0)
        parts = jnp.concatenate([p.astype(jnp.bfloat16) for p in three_parts(field)], axis=1)
        picked = jnp.dot(parts, hot_lane[...], preferred_element_type=jnp.float32)
        trace_own[s] = jnp.sum(picked * hot_row[...], axis=0, keepdims=True)

    def plane_copy(s, k):
        return pltpu.make_async_remote_copy(
            src_ref=trace_own.at[s],
            dst_ref=trace_plane.at[s, k],
            send_sem=plane_send.at[s, k],
            recv_sem=plane_recv.at[s, k],
            device_id=plane_peer(k),
            device_id_type=MESH,
        )

    def line_copy(s, k):
        return pltpu.make_async_remote_copy(
            src_ref=trace_sum.at[s],
            dst_ref=trace_line.at[s, k],
            send_sem=line_send.at[s, k],
            recv_sem=line_recv.at[s, k],
            device_id=line_peer(k),
            device_id_type=MESH,
        )

    def share_plane(s):
        for k in range(1, n_x * n_d):
            plane_copy(s, k).start()

    def share_line(s):
        total = trace_own[s]
        for k in range(1, n_x * n_d):
            plane_copy(s, k).wait_recv()
            total = total + trace_plane[s, k]
        trace_sum[s] = total
        for k in range(1, n_in):
            line_copy(s, k).start()

    def finish_trace(s):
        total = trace_sum[s]
        for k in range(1, n_in):
            line_copy(s, k).wait_recv()
            total = total + trace_line[s, k]
        traces_out[s : s + 1, :] = total

    expected = jnp.int32(n_x * n_d - 1 + n_in - 1)
    for d in crossing:
        expected = expected + jnp.where(present(d), 1, 0)
    loads[0].wait()
    stage_edges(0, 0)
    stage_rows(0, 0)
    loads[1].wait()
    stage_edges(0, 1)
    stage_rows(0, 1)
    pl.semaphore_wait(barrier, expected)
    for system in range(2):
        send(0, system, early)
        send(0, system, late)
    for load in loads[2:]:
        load.wait()
    coefficients()
    receivers()
    for s in range(STEPS):
        for system in range(2):
            receive(s, system)
            finish_halo(s, system)
            advance(s, system, outer)
            if s < STEPS - 1:
                stage_edges(s + 1, system)
                send(s + 1, system, early)
            advance(s, system, inner)
            if s < STEPS - 1:
                stage_rows(s + 1, system)
                send(s + 1, system, late)
            elif system == 0:
                sample(s)
                share_plane(s)
                share_line(s - 1)
        if s < STEPS - 1:
            sample(s)
            share_plane(s)
            if s > 0:
                share_line(s - 1)
    share_line(STEPS - 1)
    for s in range(STEPS):
        finish_trace(s)
    for s in range(STEPS):
        for system in range(2):
            drain(s, system)
        for k in range(1, n_x * n_d):
            plane_copy(s, k).wait_send()
        for k in range(1, n_in):
            line_copy(s, k).wait_send()


def publish(*refs):
    half = len(refs) // 2
    for source, place in zip(refs[:half], refs[half:]):
        place[...] = source[...]


def per_device(sizes, *operands):
    shapes = [operand.shape for operand in operands]
    _, cx, cy, cz = shapes[0]
    nrec = shapes[13][0]
    n_in, n_x, n_d = sizes
    operands = list(operands)
    for which in (9, 10, 13):
        operands[which] = operands[which].reshape(1, -1)
    f32, bf16 = jnp.float32, jnp.bfloat16
    padded = cy + 2 * TOP
    combos = 2 * cx
    scratch = [
        pltpu.VMEM((STEPS + 2, 2, 2, cx + 2, padded, cz), f32),
        pltpu.VMEM((3, cx, cy, cz), f32),
        pltpu.VMEM((2, cx, cy, cz), jnp.int32),
        pltpu.VMEM((9, cx, cy, cz), f32),
        pltpu.VMEM((2, cx + 2, padded, cz), f32),
        pltpu.VMEM((2, cx, cy, cz), f32),
        pltpu.VMEM((STEPS, 2, 2, combos, cz), f32),
        pltpu.VMEM((STEPS, 2, 2, combos, cz), f32),
        pltpu.VMEM((STEPS, 2, 2, 8, cz), f32),
        pltpu.VMEM((STEPS, 2, 2, combos, cz), f32),
        pltpu.VMEM((STEPS, 2, 2, 2, cx, cy, cz), f32),
        pltpu.VMEM((STEPS, 2, 2, 2, combos, cz), f32),
        pltpu.VMEM((STEPS, 2, 2, 2, 8, cz), f32),
        pltpu.VMEM((STEPS, 2, 2, 2, combos, cz), f32),
        pltpu.VMEM((cx * cy, nrec), f32),
        pltpu.VMEM((3 * cz, nrec), bf16),
        pltpu.VMEM((3 * STEPS * cx * cy, nrec), bf16),
        pltpu.VMEM((STEPS, cx, cy, cz), f32),
        pltpu.VMEM((STEPS, 1, nrec), f32),
        pltpu.VMEM((STEPS, n_x * n_d, 1, nrec), f32),
        pltpu.VMEM((STEPS, 1, nrec), f32),
        pltpu.VMEM((STEPS, n_in, 1, nrec), f32),
        pltpu.SemaphoreType.DMA((9,)),
        pltpu.SemaphoreType.DMA((STEPS, 2, len(DIRECTIONS))),
        pltpu.SemaphoreType.DMA((STEPS, 2, len(DIRECTIONS))),
        pltpu.SemaphoreType.DMA((STEPS, n_x * n_d)),
        pltpu.SemaphoreType.DMA((STEPS, n_x * n_d)),
        pltpu.SemaphoreType.DMA((STEPS, n_in)),
        pltpu.SemaphoreType.DMA((STEPS, n_in)),
    ]
    vmem = pl.BlockSpec(memory_space=pltpu.VMEM)
    smem = pl.BlockSpec(memory_space=pltpu.SMEM)
    anywhere = pl.BlockSpec(memory_space=pl.ANY)
    made = pl.pallas_call(
        functools.partial(kernel, sizes),
        out_shape=(
            jax.ShapeDtypeStruct((2, cx, cy, cz), f32),
            jax.ShapeDtypeStruct((2, cx, cy, cz), f32),
            jax.ShapeDtypeStruct((cx, cy, cz), f32),
            jax.ShapeDtypeStruct((STEPS, nrec), f32),
        ),
        in_specs=[anywhere] * 9 + [vmem, vmem, smem, smem, vmem, vmem],
        out_specs=(vmem, vmem, vmem, vmem),
        scratch_shapes=scratch,
        compiler_params=pltpu.CompilerParams(
            collective_id=0, has_side_effects=True, vmem_limit_bytes=56 * 2**20
        ),
        name="wavefields",
    )(*operands)
    return pl.pallas_call(
        publish,
        out_shape=[jax.ShapeDtypeStruct(m.shape, m.dtype) for m in made],
        in_specs=[vmem] * len(made),
        out_specs=[vmem] * len(made),
        name="publish",
    )(*made)


def solution(mesh):
    sizes = tuple(mesh.shape[axis] for axis in AXES)
    field = P(None, ("shot", "inline"), "xline", "depth")
    cell = P("inline", "xline", "depth")
    return jax.shard_map(
        functools.partial(per_device, sizes),
        mesh=mesh,
        in_specs=(
            field, field, field, field,
            cell, cell, cell, cell, cell,
            P(), P(), P("shot"), P("shot"), P("shot"), P(None, "shot"),
        ),
        out_specs=(field, field, P(("shot", "inline"), "xline", "depth"), P(None, "shot")),
        check_vma=False,
    )
```
